8 devices in a mesh: replica: 2 (over z, y), stage: 4 (over x, core).
Axes of the slice: x: 2, y: 2, z: 1, core: 2. Of those that a mesh axis runs over, the one named last changes fastest.
Arguments:
- embeddings: bfloat16 [8192, 3072], P('replica'), parts along dimension 0
- valid_len: int32 [2], P('replica'), parts along dimension 0
- attn_gain: float32 [4, 3072], P('stage')
- w_q: bfloat16 [4, 3072, 24, 128], P('stage')
- w_k: bfloat16 [4, 3072, 8, 128], P('stage')
- w_v: bfloat16 [4, 3072, 8, 128], P('stage')
- w_o: bfloat16 [4, 24, 128, 3072], P('stage')
- mlp_gain: float32 [4, 3072], P('stage')
- w_gate: bfloat16 [4, 3072, 8192], P('stage')
- w_up: bfloat16 [4, 3072, 8192], P('stage')
- w_down: bfloat16 [4, 8192, 3072], P('stage')
Outputs:
- output 1: bfloat16 [8192, 3072], P(('replica', 'stage')), parts along dimension 0
- output 2: bfloat16 [4, 8192, 8, 128], P('stage', 'replica'), parts along dimension 1
- output 3: bfloat16 [4, 8192, 8, 128], P('stage', 'replica'), parts along dimension 1
There are 2 independent parts. The reference program is written for one: setup_inputs(seed, part) draws one part's arguments, and reference() takes and returns one part's arrays. A program takes and returns all parts, laid end to end along the dimension named above; an argument that names none is the same for every part.
All inputs are finite; a program needn't handle non-finite values.
Results may differ from the reference program's by a relative error of at most 0.02.
Values are sent between devices in bfloat16 or wider.
A program may use at most 1 GiB of HBM per device.

```python
import jax
import jax.numpy as jnp
from jax import lax

D = 3072
HEADS = 24
KV_HEADS = 8
HEAD = 128
FF = 8192
LAYERS = 4
SEQ = 4096

GROUP = HEADS // KV_HEADS
HALF = HEAD // 2
QBLOCK = min(SEQ, 128)
EPS = 1e-5
ROPE_BASE = 10000.0
NEG_BIG = -1e30


def setup_inputs(seed: int = 0, part: int = 0) -> dict:
    part_key = jax.random.fold_in(jax.random.key(seed), part)
    embed_key, len_key = jax.random.split(part_key)
    weight_keys = jax.random.split(jax.random.key(seed + 1), 9)

    def normal_weight(draw_key, arr_shape, std_scale):
        return (jax.random.normal(draw_key, arr_shape, jnp.float32) * std_scale).astype(jnp.bfloat16)

    embeddings = jax.random.normal(embed_key, (SEQ, D), jnp.float32).astype(jnp.bfloat16)
    valid_len = jax.random.randint(len_key, (1,), SEQ // 2, SEQ - SEQ // 8 + 1, jnp.int32)
    return {
        'embeddings': embeddings,
        'valid_len': valid_len,
        'attn_gain': jax.random.uniform(weight_keys[0], (LAYERS, D), jnp.float32, 0.6, 1.4),
        'w_q': normal_weight(weight_keys[1], (LAYERS, D, HEADS, HEAD), 2.0 * D ** -0.5),
        'w_k': normal_weight(weight_keys[2], (LAYERS, D, KV_HEADS, HEAD), D ** -0.5),
        'w_v': normal_weight(weight_keys[3], (LAYERS, D, KV_HEADS, HEAD), D ** -0.5),
        'w_o': normal_weight(weight_keys[4], (LAYERS, HEADS, HEAD, D), (HEADS * HEAD) ** -0.5),
        'mlp_gain': jax.random.uniform(weight_keys[5], (LAYERS, D), jnp.float32, 0.6, 1.4),
        'w_gate': normal_weight(weight_keys[6], (LAYERS, D, FF), D ** -0.5),
        'w_up': normal_weight(weight_keys[7], (LAYERS, D, FF), D ** -0.5),
        'w_down': normal_weight(weight_keys[8], (LAYERS, FF, D), FF ** -0.5),
    }


def rms_norm(hidden, norm_gain):
    hid32 = hidden.astype(jnp.float32)
    inv_rms = lax.rsqrt(jnp.mean(hid32 * hid32, axis=-1, keepdims=True) + EPS)
    return (hid32 * inv_rms * norm_gain).astype(jnp.bfloat16)


def apply_rope(values, cos_tab, sin_tab):
    front_half = values[..., :HALF]
    back_half = values[..., HALF:]
    return jnp.concatenate([front_half * cos_tab - back_half * sin_tab, back_half * cos_tab + front_half * sin_tab], axis=-1)


def reference(embeddings, valid_len, attn_gain, w_q, w_k, w_v, w_o, mlp_gain, w_gate, w_up, w_down):
    positions = jnp.arange(SEQ)
    inv_freq = ROPE_BASE ** (-jnp.arange(HALF).astype(jnp.float32) * (2.0 / HEAD))
    angles = positions.astype(jnp.float32)[:, None] * inv_freq[None, :]
    cos_tab = jnp.cos(angles)[:, None, :]
    sin_tab = jnp.sin(angles)[:, None, :]
    key_ok = positions < valid_len[0]
    n_blocks = SEQ // QBLOCK

    def layer_fn(hidden, layer_params):
        a_gain, wq_l, wk_l, wv_l, wo_l, m_gain, wg_l, wu_l, wd_l = layer_params
        normed = rms_norm(hidden, a_gain).astype(jnp.float32)
        q_proj = jnp.einsum('sd,dhk->shk', normed, wq_l.astype(jnp.float32))
        k_proj = jnp.einsum('sd,dhk->shk', normed, wk_l.astype(jnp.float32))
        v_new = jnp.einsum('sd,dhk->shk', normed, wv_l.astype(jnp.float32)).astype(jnp.bfloat16)
        q_rot = apply_rope(q_proj, cos_tab, sin_tab).astype(jnp.bfloat16)
        k_rot = apply_rope(k_proj, cos_tab, sin_tab).astype(jnp.bfloat16)
        q_blocks = q_rot.astype(jnp.float32).reshape(n_blocks, QBLOCK, KV_HEADS, GROUP, HEAD)
        k_all = k_rot.astype(jnp.float32)
        v_all = v_new.astype(jnp.float32)

        def attend(block_in):
            block_idx, q_block = block_in
            q_pos = block_idx * QBLOCK + jnp.arange(QBLOCK)
            scores = jnp.einsum('qhgd,khd->hgqk', q_block, k_all) * (HEAD ** -0.5)
            allowed = (positions[None, :] <= q_pos[:, None]) & key_ok[None, :]
            scores = jnp.where(allowed, scores, NEG_BIG)
            probs_all = jax.nn.softmax(scores, axis=-1).astype(jnp.bfloat16).astype(jnp.float32)
            return jnp.einsum('hgqk,khd->qhgd', probs_all, v_all).astype(jnp.bfloat16)

        attn_heads = lax.map(attend, (jnp.arange(n_blocks), q_blocks)).reshape(SEQ, HEADS, HEAD)
        attn_out = jnp.einsum('shk,hkd->sd', attn_heads.astype(jnp.float32), wo_l.astype(jnp.float32))
        hidden = (hidden.astype(jnp.float32) + attn_out).astype(jnp.bfloat16)
        normed = rms_norm(hidden, m_gain)
        gate_proj = jnp.dot(normed, wg_l, preferred_element_type=jnp.float32)
        up_proj = jnp.dot(normed, wu_l, preferred_element_type=jnp.float32)
        act_val = (jax.nn.silu(gate_proj) * up_proj).astype(jnp.bfloat16)
        down_proj = jnp.dot(act_val, wd_l, preferred_element_type=jnp.float32)
        hidden = (hidden.astype(jnp.float32) + down_proj).astype(jnp.bfloat16)
        return hidden, (k_rot, v_new)

    hidden_out, caches = lax.scan(layer_fn, embeddings, (attn_gain, w_q, w_k, w_v, w_o, mlp_gain, w_gate, w_up, w_down))
    return hidden_out, caches[0], caches[1]
```

```python
import functools
import jax
import jax.numpy as jnp
from jax import lax
from jax.experimental import pallas as pl
from jax.experimental.pallas import tpu as pltpu
from jax.sharding import PartitionSpec as P

EPS = 1e-5
ROPE_BASE = 10000.0
NEG_BIG = -1e30
LOG2E = 1.4426950408889634
BLK = 256
KB = 512
WC = 512
DC = 256
NS = 6
NG = 3
ND = 4


def normed(hidden, gain):
    hid32 = hidden.astype(jnp.float32)
    inv_rms = lax.rsqrt(jnp.mean(hid32 * hid32, axis=-1, keepdims=True) + EPS)
    return (hid32 * inv_rms * gain).astype(jnp.bfloat16)


def dot(a, b):
    return jnp.dot(a, b, preferred_element_type=jnp.float32)


def alloc_kernel(*refs):
    pass


def attn_kernel(tick, base, emb, recv, gain, cos_hbm, sin_hbm, wq, wk, wv, wo, fin, hlast, kt_in, vw_in, kc_in, vc_in, out_in,
                h1, staged, kt, vw, kc, vc, out,
                hin, a, qs, knt, vn, kvf, kst, vst, ob, relay, wbuf, ktbuf, vbuf, cosb, sinb, s_a, s_b, m_a, m_b, l_s, acc_s,
                wsem, ksem, vsem, hsem, csem, osem, fsem):
    valid, stage = base[0], base[1]
    stages = base[2]
    d_model = wq.shape[0]
    kv_heads, head_dim, seq_len = kt.shape
    group = wq.shape[1] // (kv_heads * head_dim)
    rows3 = group * BLK
    n_blocks = seq_len // BLK
    per_owner = out.shape[0] // BLK
    per = WC // head_dim
    n_q, n_k, n_o = wq.shape[1] // WC, wk.shape[1] // WC, wo.shape[1] // WC
    max_kb = s_a.shape[0]
    bounds = [(0, wq), (n_q, wk), (n_q + n_k, wv), (n_q + 2 * n_k, wo)]
    total = n_q + 2 * n_k + n_o
    ends = [b[0] for b in bounds[1:]] + [total]
    scale2 = head_dim ** -0.5 * LOG2E
    blk_raw = tick[0] - stage
    blk = jnp.clip(blk_raw, 0, n_blocks - 1)
    active = (blk_raw >= 0) & (blk_raw < n_blocks)
    is_last = stage == stages - 1

    def wcopy(ref, col, slot):
        return pltpu.make_async_copy(ref.at[:, pl.ds(pl.multiple_of(col * WC, WC), WC)], wbuf.at[slot], wsem.at[slot])

    def wstart(c):
        for (lo, ref), hi in zip(bounds, ends):
            if isinstance(c, int):
                if lo <= c < hi:
                    wcopy(ref, c - lo, c % NS).start()
            else:
                @pl.when((c >= lo) & (c < hi))
                def _():
                    wcopy(ref, c - lo, lax.rem(c, NS)).start()

    def wwait(c):
        wcopy(wq, 0, lax.rem(c, NS)).wait()

    pos = pl.multiple_of(blk * BLK, BLK)
    nkb = jnp.minimum(jnp.minimum((pos + BLK + KB - 1) // KB, (valid + KB - 1) // KB), max_kb)
    nfull = jnp.minimum((pos + 1) // KB, valid // KB)

    def emb_copy():
        return pltpu.make_async_copy(emb.at[pl.ds(pos, BLK), :], hin, hsem.at[0])

    def recv_copy(i):
        return pltpu.make_async_copy(recv.at[i], hin.at[:, pl.ds(i * DC, DC)], hsem.at[i])

    @pl.when(active & (stage == 0))
    def _():
        emb_copy().start()

    @pl.when(active & (stage != 0))
    def _():
        for i in range(d_model // DC):
            recv_copy(i).start()

    ccopy = pltpu.make_async_copy(cos_hbm.at[pl.ds(pos, BLK), :], cosb, csem.at[0])
    scopy = pltpu.make_async_copy(sin_hbm.at[pl.ds(pos, BLK), :], sinb, csem.at[1])

    def kt_copy(h, slot, kb):
        return pltpu.make_async_copy(kt.at[h, :, pl.ds(pl.multiple_of(kb * KB, KB), KB)], ktbuf.at[slot, kb], ksem.at[slot, kb])

    def v_copy(h, slot, kb):
        rows = pl.ds(pl.multiple_of(kb * KB, KB), KB)
        return pltpu.make_async_copy(vw.at[h, rows, :], vbuf.at[slot, rows, :], vsem.at[slot, kb])

    def over_kb(make, h, slot, act):
        def body(kb, carry):
            getattr(make(h, slot, kb), act)()
            return carry
        lax.fori_loop(0, nkb, body, 0)

    @pl.when(active)
    def _():
        ccopy.start()
        scopy.start()
        for c in range(NS):
            wstart(c)
        over_kb(kt_copy, 0, 0, 'start')
        over_kb(v_copy, 0, 0, 'start')
        over_kb(kt_copy, 1, 1, 'start')

    done_blk = jnp.where(is_last, tick[0] - stages, tick[0] - stages - 1)
    own_row = done_blk - stage * per_owner
    mine = (own_row >= 0) & (own_row < per_owner)
    own_row = pl.multiple_of(jnp.clip(own_row, 0, per_owner - 1) * BLK, BLK)
    relay_in = pltpu.make_async_copy(hlast, relay, fsem.at[0])
    relay_fin = pltpu.make_async_copy(fin, relay, fsem.at[0])
    relay_stage = pltpu.make_async_copy(relay, staged, fsem.at[1])
    relay_out = pltpu.make_async_copy(relay, out.at[pl.ds(own_row, BLK), :], fsem.at[2])

    mine = mine & active
    last_active = is_last & active
    fin_active = mine & jnp.logical_not(is_last)

    @pl.when(last_active)
    def _():
        relay_in.start()

    @pl.when(fin_active)
    def _():
        relay_fin.start()

    @pl.when(active & (stage == 0))
    def _():
        emb_copy().wait()

    @pl.when(active & (stage != 0))
    def _():
        for i in range(d_model // DC):
            recv_copy(i).wait()

    @pl.when(active)
    def _():
        a[...] = normed(hin[...], gain[...])
        ccopy.wait()
        scopy.wait()

        def rope(x):
            return x * cosb[...] + pltpu.roll(x, head_dim // 2, 1) * sinb[...]

        def pair_of(lhs, j, use):
            c = 2 * j
            wwait(c)
            wwait(c + 1)
            accs = [dot(lhs[...], wbuf[lax.rem(c + i, NS)]) for i in range(2)]
            for i in range(2):
                use(c + i, accs[i])

        def q_use(c, acc):
            for i in range(per):
                qs[c * per + i] = rope(acc[:, i * head_dim:(i + 1) * head_dim]).astype(jnp.bfloat16)

        def k_use(c, acc):
            for i in range(per):
                h = (c - n_q) * per + i
                x = rope(acc[:, i * head_dim:(i + 1) * head_dim])
                kvf[pl.ds(h, BLK, stride=kv_heads), :] = x
                knt[h] = x.T.astype(jnp.bfloat16)

        def v_use(c, acc):
            for i in range(per):
                h = (c - n_q - n_k) * per + i
                x = acc[:, i * head_dim:(i + 1) * head_dim]
                kvf[pl.ds(h, BLK, stride=kv_heads), :] = x
                vn[h] = x.astype(jnp.bfloat16)

        def project(use):
            def body(j, carry):
                pair_of(a, j, use)
                wstart(2 * j + NS)
                wstart(2 * j + 1 + NS)
                return carry
            return body

        q_step, k_step, v_step = project(q_use), project(k_use), project(v_use)

        cache_rows = pl.ds(pl.multiple_of(pos * kv_heads, BLK), BLK * kv_heads)
        k_out = pltpu.make_async_copy(kst, kc.at[cache_rows, :], osem.at[0])
        v_out = pltpu.make_async_copy(vst, vc.at[cache_rows, :], osem.at[1])
        kt_out = pltpu.make_async_copy(knt, kt.at[:, :, pl.ds(pos, BLK)], osem.at[2])
        vw_out = pltpu.make_async_copy(vn, vw.at[:, pl.ds(pos, BLK), :], osem.at[3])

        lax.fori_loop(0, n_q // 2, q_step, 0)
        lax.fori_loop(n_q // 2, (n_q + n_k) // 2, k_step, 0)
        kst[...] = kvf[...].astype(jnp.bfloat16)
        k_out.start()
        lax.fori_loop((n_q + n_k) // 2, (n_q + 2 * n_k) // 2, v_step, 0)
        vst[...] = kvf[...].astype(jnp.bfloat16)
        v_out.start()

        @pl.when(last_active)
        def _():
            relay_in.wait()
            relay_stage.start()

        @pl.when(fin_active)
        def _():
            relay_fin.wait()

        @pl.when(mine)
        def _():
            relay_out.start()

        has_self = pos < nkb * KB
        self_kb = pos // KB
        self_off = pl.multiple_of(pos - self_kb * KB, BLK)

        def patch_k(h, slot):
            over_kb(kt_copy, h, slot, 'wait')

            @pl.when(has_self)
            def _():
                ktbuf[slot, self_kb, :, pl.ds(self_off, BLK)] = knt[h]

        def patch_v(h, slot):
            over_kb(v_copy, h, slot, 'wait')

            @pl.when(has_self)
            def _():
                vbuf[slot, pl.ds(pos, BLK), :] = vn[h]

            @pl.when(has_self & (self_off == 0))
            def _():
                vbuf[slot, pl.ds(pl.multiple_of(pos + BLK, BLK), KB - BLK), :] = jnp.zeros((KB - BLK, head_dim), jnp.bfloat16)

        def qk(h, slot, kb, s_ref, m_ref, masked):
            s = dot(qs[pl.ds(h * group, group)].reshape(rows3, head_dim), ktbuf[slot, kb])
            if masked:
                q_pos = pos + (lax.broadcasted_iota(jnp.int32, (rows3, KB), 0) & (BLK - 1))
                k_pos = kb * KB + lax.broadcasted_iota(jnp.int32, (rows3, KB), 1)
                s = jnp.where((k_pos <= q_pos) & (k_pos < valid), s, NEG_BIG)
            s = s * scale2
            s_ref[kb] = s
            parts = [s[:, i:i + head_dim] for i in range(0, KB, head_dim)]
            m_ref[...] = jnp.maximum(m_ref[...], functools.reduce(jnp.maximum, parts))

        def pv(slot, kb, s_ref, m_ref):
            top = m_ref[...]
            probs = [jnp.exp2(s_ref[kb, :, i:i + head_dim] - top) for i in range(0, KB, head_dim)]
            l_s[...] += functools.reduce(jnp.add, probs)
            pb = jnp.concatenate([x.astype(jnp.bfloat16) for x in probs], axis=1)
            acc_s[...] += dot(pb, vbuf[slot, pl.ds(pl.multiple_of(kb * KB, KB), KB), :])

        def begin(m_ref):
            m_ref[...] = jnp.full(m_ref.shape, NEG_BIG, jnp.float32)

        def top_of(m_ref):
            m_ref[...] = jnp.broadcast_to(jnp.max(m_ref[...], axis=-1, keepdims=True), m_ref.shape)
            l_s[...] = jnp.zeros(l_s.shape, jnp.float32)
            acc_s[...] = jnp.zeros(acc_s.shape, jnp.float32)

        def finish(h):
            o = acc_s[...] / jnp.sum(l_s[...], axis=-1, keepdims=True)
            for g in range(group):
                cols = pl.ds(pl.multiple_of((h * group + g) * head_dim, head_dim), head_dim)
                ob[:, cols] = o[g * BLK:(g + 1) * BLK].astype(jnp.bfloat16)

        def loops(full, edge):
            def full_body(kb, carry):
                full(kb)
                return carry

            def edge_body(kb, carry):
                edge(kb)
                return carry
            def two_body(i, carry):
                full(2 * i)
                full(2 * i + 1)
                return carry
            lax.fori_loop(0, nfull // 2, two_body, 0)
            lax.fori_loop(nfull - lax.rem(nfull, 2), nfull, full_body, 0)
            lax.fori_loop(nfull, nkb, edge_body, 0)

        def both(h, parity, prefetch):
            s_now, m_now, s_next, m_next = (s_a, m_a, s_b, m_b) if parity == 0 else (s_b, m_b, s_a, m_a)
            if prefetch:
                over_kb(kt_copy, h + 2, parity, 'start')
            over_kb(v_copy, h + 1, 1 - parity, 'start')
            patch_k(h + 1, 1 - parity)
            patch_v(h, parity)
            top_of(m_now)
            begin(m_next)

            def run(kb, masked):
                qk(h + 1, 1 - parity, kb, s_next, m_next, masked)
                pv(parity, kb, s_now, m_now)
            loops(lambda kb: run(kb, False), lambda kb: run(kb, True))
            finish(h)

        patch_k(0, 0)
        begin(m_a)
        loops(lambda kb: qk(0, 0, kb, s_a, m_a, False), lambda kb: qk(0, 0, kb, s_a, m_a, True))

        def pair(i, carry):
            both(2 * i, 0, True)
            both(2 * i + 1, 1, True)
            return carry

        lax.fori_loop(0, kv_heads // 2 - 1, pair, 0)
        both(kv_heads - 2, 0, False)
        patch_v(kv_heads - 1, 1)
        top_of(m_b)
        lax.fori_loop(0, nkb, lambda kb, carry: (pv(1, kb, s_b, m_b), carry)[1], 0)
        finish(kv_heads - 1)
        kt_out.start()
        vw_out.start()

        def o_use(c, acc):
            cols = pl.ds(pl.multiple_of((c - (total - n_o)) * WC, WC), WC)
            h1[:, cols] = (hin[:, cols].astype(jnp.float32) + acc).astype(jnp.bfloat16)

        lax.fori_loop((total - n_o) // 2, total // 2, lambda j, carry: (pair_of(ob, j, o_use), carry)[1], 0)
        k_out.wait()
        v_out.wait()
        kt_out.wait()
        vw_out.wait()

    @pl.when(last_active)
    def _():
        relay_stage.wait()

    @pl.when(mine)
    def _():
        relay_out.wait()


def mlp_kernel(stages, h1, gain, staged, wg, wu, wd, hout, recv, fin, b, act, hbuf, gbuf, ubuf, dbuf, gsem, usem, dsem, ssem, rsem, fssem, frsem):
    stage = lax.axis_index('stage')
    d_ff = wg.shape[1]
    n_g, n_d = d_ff // WC, wd.shape[1] // DC
    barrier = pltpu.get_barrier_semaphore()

    @pl.when(stage > 0)
    def _():
        pl.semaphore_signal(barrier, inc=1, device_id={'stage': stage - 1}, device_id_type=pl.DeviceIdType.MESH)

    @pl.when(stage < stages - 1)
    def _():
        pl.semaphore_signal(barrier, inc=1, device_id={'stage': stages - 1}, device_id_type=pl.DeviceIdType.MESH)

    def deliver(i):
        return pltpu.make_async_remote_copy(src_ref=staged, dst_ref=fin, send_sem=fssem.at[i], recv_sem=frsem.at[0],
                                            device_id={'stage': i}, device_id_type=pl.DeviceIdType.MESH)

    def gu_copies(c, slot):
        cols = pl.ds(pl.multiple_of(c * WC, WC), WC)
        return (pltpu.make_async_copy(wg.at[:, cols], gbuf.at[slot], gsem.at[slot]),
                pltpu.make_async_copy(wu.at[:, cols], ubuf.at[slot], usem.at[slot]))

    def d_copy(c, slot):
        return pltpu.make_async_copy(wd.at[:, pl.ds(pl.multiple_of(c * DC, DC), DC)], dbuf.at[slot], dsem.at[slot])

    for c in range(NG):
        for cp in gu_copies(c, c):
            cp.start()
    b[...] = normed(h1[...], gain[...])

    def gate_up(c, carry):
        slot = lax.rem(c, NG)

        @pl.when((c == 1) & (stage < stages - 1))
        def _():
            pl.semaphore_wait(barrier, 1)

        @pl.when((c == 1) & (stage == stages - 1))
        def _():
            pl.semaphore_wait(barrier, stages - 1)
            for i in range(stages - 1):
                deliver(i).start()

        for cp in gu_copies(c, slot):
            cp.wait()
        gate = dot(b[...], gbuf[slot])
        up = dot(b[...], ubuf[slot])
        act[:, pl.ds(pl.multiple_of(c * WC, WC), WC)] = (jax.nn.silu(gate) * up).astype(jnp.bfloat16)

        @pl.when(c + NG < n_g)
        def _():
            for cp in gu_copies(c + NG, slot):
                cp.start()

        @pl.when(c >= n_g - ND)
        def _():
            d_copy(c - (n_g - ND), c - (n_g - ND)).start()
        return carry

    lax.fori_loop(0, n_g, gate_up, 0)

    def send(c):
        return pltpu.make_async_remote_copy(src_ref=hbuf.at[c], dst_ref=recv.at[c], send_sem=ssem.at[c], recv_sem=rsem.at[c],
                                            device_id={'stage': lax.rem(stage + 1, stages)}, device_id_type=pl.DeviceIdType.MESH)

    def down(c, carry):
        slot = lax.rem(c, ND)
        d_copy(c, slot).wait()
        cols = pl.ds(pl.multiple_of(c * DC, DC), DC)
        y = (h1[:, cols].astype(jnp.float32) + dot(act[...], dbuf[slot])).astype(jnp.bfloat16)
        hbuf[c] = y
        hout[:, cols] = y

        @pl.when(c + ND < n_d)
        def _():
            d_copy(c + ND, slot).start()

        @pl.when(stage < stages - 1)
        def _():
            send(c).start()
        return carry

    lax.fori_loop(0, n_d, down, 0)

    @pl.when(stage < stages - 1)
    def _():
        for c in range(n_d):
            send(c).wait_send()
        deliver(0).wait_recv()

    @pl.when(stage == stages - 1)
    def _():
        for i in range(stages - 1):
            deliver(i).wait_send()

    @pl.when(stage > 0)
    def _():
        for c in range(n_d):
            send(c).wait_recv()


def solution(mesh):
    stages = mesh.shape['stage']
    gain_spec = P('stage', None)
    spec_three = P('stage', None, None)
    spec_four = P('stage', None, None, None)
    any_spec = pl.BlockSpec(memory_space=pl.ANY)
    vmem_spec = pl.BlockSpec(memory_space=pltpu.VMEM)
    smem_spec = pl.BlockSpec(memory_space=pltpu.SMEM)
    bf16, f32 = jnp.bfloat16, jnp.float32

    def stage_program(embeddings, valid_len, attn_gain, w_q, w_k, w_v, w_o, mlp_gain, w_gate, w_up, w_down):
        seq_len, d_model = embeddings.shape
        kv_heads, head_dim = w_k.shape[2], w_k.shape[3]
        heads = w_q.shape[2]
        group = heads // kv_heads
        d_ff = w_gate.shape[2]
        n_blocks = seq_len // BLK
        per_owner = n_blocks // stages
        n_d = d_model // DC
        stage = lax.axis_index('stage')

        wq = w_q[0].reshape(d_model, heads * head_dim)
        wk = w_k[0].reshape(d_model, kv_heads * head_dim)
        wv = w_v[0].reshape(d_model, kv_heads * head_dim)
        wo = w_o[0].reshape(heads * head_dim, d_model)
        wg, wu, wd = w_gate[0], w_up[0], w_down[0]

        half = head_dim // 2
        inv_freq = ROPE_BASE ** (-jnp.arange(half, dtype=f32) * (2.0 / head_dim))
        angles = jnp.arange(seq_len).astype(f32)[:, None] * inv_freq[None, :]
        cos_tab, sin_tab = jnp.cos(angles), jnp.sin(angles)
        cos_full = jnp.concatenate([cos_tab, cos_tab], axis=1)
        sin_full = jnp.concatenate([-sin_tab, sin_tab], axis=1)

        max_kb = -(-(seq_len - seq_len // 8) // KB)
        rows3 = group * BLK
        hid = jax.ShapeDtypeStruct((BLK, d_model), bf16)
        chunks = jax.ShapeDtypeStruct((n_d, BLK, DC), bf16)
        kt_t = jax.ShapeDtypeStruct((kv_heads, head_dim, seq_len), bf16)
        vw_t = jax.ShapeDtypeStruct((kv_heads, seq_len, head_dim), bf16)
        cache_t = jax.ShapeDtypeStruct((seq_len * kv_heads, head_dim), bf16)
        out_t = jax.ShapeDtypeStruct((per_owner * BLK, d_model), bf16)

        def vmem(*shape, dtype=bf16):
            return pltpu.VMEM(shape, dtype)

        def dma(*shape):
            return pltpu.SemaphoreType.DMA(shape)

        attn_call = pl.pallas_call(
            attn_kernel,
            out_shape=(hid, hid, kt_t, vw_t, cache_t, cache_t, out_t),
            in_specs=[smem_spec, smem_spec, any_spec, any_spec, vmem_spec] + [any_spec] * 13,
            out_specs=(vmem_spec,) + (any_spec,) * 6,
            input_output_aliases={13: 2, 14: 3, 15: 4, 16: 5, 17: 6},
            scratch_shapes=[
                vmem(BLK, d_model), vmem(BLK, d_model), vmem(heads, BLK, head_dim),
                vmem(kv_heads, head_dim, BLK), vmem(kv_heads, BLK, head_dim),
                vmem(BLK * kv_heads, head_dim, dtype=f32), vmem(BLK * kv_heads, head_dim), vmem(BLK * kv_heads, head_dim),
                vmem(BLK, d_model), vmem(BLK, d_model),
                vmem(NS, d_model, WC),
                vmem(2, max_kb, head_dim, KB), vmem(2, max_kb * KB, head_dim),
                vmem(BLK, head_dim, dtype=f32), vmem(BLK, head_dim, dtype=f32),
                vmem(max_kb, rows3, KB, dtype=f32), vmem(max_kb, rows3, KB, dtype=f32),
                vmem(rows3, head_dim, dtype=f32), vmem(rows3, head_dim, dtype=f32),
                vmem(rows3, head_dim, dtype=f32), vmem(rows3, head_dim, dtype=f32),
                dma(NS), dma(2, max_kb), dma(2, max_kb), dma(n_d), dma(2), dma(4), dma(3),
            ],
            compiler_params=pltpu.CompilerParams(vmem_limit_bytes=62 * 1024 * 1024),
            cost_estimate=pl.CostEstimate(flops=2 * BLK * d_model * (2 * d_model + 2 * kv_heads * head_dim),
                                          bytes_accessed=60 * 1024 * 1024, transcendentals=0),
            name='attn_block',
        )
        mlp_call = pl.pallas_call(
            functools.partial(mlp_kernel, stages),
            out_shape=(hid, chunks, hid),
            in_specs=[vmem_spec, vmem_spec, any_spec, any_spec, any_spec, any_spec],
            out_specs=(vmem_spec, any_spec, any_spec),
            scratch_shapes=[
                vmem(BLK, d_model), vmem(BLK, d_ff), vmem(n_d, BLK, DC),
                vmem(NG, d_model, WC), vmem(NG, d_model, WC), vmem(ND, d_ff, DC),
                dma(NG), dma(NG), dma(ND), dma(n_d), dma(n_d), dma(stages - 1), dma(1),
            ],
            compiler_params=pltpu.CompilerParams(vmem_limit_bytes=60 * 1024 * 1024, collective_id=0, has_side_effects=True),
            cost_estimate=pl.CostEstimate(flops=6 * BLK * d_model * d_ff, bytes_accessed=160 * 1024 * 1024, transcendentals=0),
            name='mlp_block',
        )
        init = pl.pallas_call(alloc_kernel, out_shape=(chunks, hid, hid, kt_t, vw_t, cache_t, cache_t, out_t),
                              out_specs=(any_spec,) * 8, name='buffers')()
        base = jnp.stack([valid_len[0], stage, jnp.int32(stages)]).astype(jnp.int32)

        def tick(tick_idx, state):
            recv, fin, hlast, kt, vw, kc, vc, out = state
            h1, staged, kt, vw, kc, vc, out = attn_call(tick_idx.reshape(1), base, embeddings, recv, attn_gain, cos_full, sin_full,
                                                        wq, wk, wv, wo, fin, hlast, kt, vw, kc, vc, out)
            hlast, recv, fin = mlp_call(h1, mlp_gain, staged, wg, wu, wd)
            return recv, fin, hlast, kt, vw, kc, vc, out

        recv, fin, hlast, kt, vw, kc, vc, out = lax.fori_loop(0, n_blocks + stages - 1, tick, tuple(init))
        row = (per_owner - 1) * BLK
        out = lax.dynamic_update_slice(out, jnp.where(stage == stages - 1, hlast, out[row:]), (row, 0))
        cache_shape = (1, seq_len, kv_heads, head_dim)
        return out, kc.reshape(cache_shape), vc.reshape(cache_shape)

    return jax.shard_map(stage_program, mesh=mesh,
                         in_specs=(P('replica', None), P('replica'), gain_spec, spec_four, spec_four, spec_four, spec_four,
                                   gain_spec, spec_three, spec_three, spec_three),
                         out_specs=(P(('replica', 'stage'), None), P('stage', 'replica', None, None), P('stage', 'replica', None, None)),
                         check_vma=False)
```
